32 devices in a mesh: dp: 2 (over x), ep: 16 (over z, y, core).
Axes of the slice: x: 2, y: 2, z: 4, core: 2. Of those that a mesh axis runs over, the one named last changes fastest.
Arguments:
- tokens: bfloat16 [8192, 2048], P(('dp', 'ep')), parts along dimension 0
- expert_ids: int32 [8192, 6], P(('dp', 'ep')), parts along dimension 0
- gate_vals: float32 [8192, 6], P(('dp', 'ep')), parts along dimension 0
- w_gate: bfloat16 [64, 2048, 1408], P('ep')
- w_up: bfloat16 [64, 2048, 1408], P('ep')
- w_down: bfloat16 [64, 1408, 2048], P('ep')
Outputs:
- output: bfloat16 [8192, 2048], P(('dp', 'ep')), parts along dimension 0
There are 2 independent parts. The reference program is written for one: setup_inputs(seed, part) draws one part's arguments, and reference() takes and returns one part's arrays. A program takes and returns all parts, laid end to end along the dimension named above; an argument that names none is the same for every part.
All inputs are finite; a program needn't handle non-finite values.
Results may differ from the reference program's by a relative error of at most 0.00666288.
Values are sent between devices in bfloat16 or wider.
A program may use at most 1 GiB of HBM per device.

```python
import jax
import jax.numpy as jnp
from jax import lax

D_MODEL = 2048
FFN_DIM = 1408
NUM_EXPERTS = 64
TOP_K = 6
GROUP = 16
TOK_DEV = 256

DEV_LIMIT = TOP_K // 2
LOCAL_EXPERTS = NUM_EXPERTS // GROUP
PAIR_CAP = TOK_DEV * DEV_LIMIT // GROUP
EXPERT_CAP = TOK_DEV * TOP_K * GROUP // NUM_EXPERTS
TOKENS = GROUP * TOK_DEV


def perm_rows(rand_key, row_count, perm_size):
    return jax.vmap(lambda sub_key: jax.random.permutation(sub_key, perm_size))(jax.random.split(rand_key, row_count))


def draw_routing(rand_key):
    key_src, key_dst, key_slot = jax.random.split(rand_key, 3)
    src_perm = perm_rows(key_src, GROUP, GROUP)
    dst_perm = perm_rows(key_dst, GROUP, LOCAL_EXPERTS)
    flat_pos = jnp.arange(TOK_DEV)[:, None] * DEV_LIMIT + jnp.arange(DEV_LIMIT)[None, :]
    dest_dev = src_perm[:, flat_pos % GROUP]
    recv_row = jnp.arange(GROUP)[:, None, None] * PAIR_CAP + (flat_pos // GROUP)[None, :, :]
    first_loc = dst_perm[dest_dev, (2 * recv_row) % LOCAL_EXPERTS]
    second_loc = dst_perm[dest_dev, (2 * recv_row + 1) % LOCAL_EXPERTS]
    pair_ids = jnp.stack([first_loc, second_loc], axis=-1) + dest_dev[..., None] * LOCAL_EXPERTS
    ordered = pair_ids.reshape(TOKENS, TOP_K)
    scores = jax.random.randint(key_slot, (TOKENS, TOP_K), 0, 1 << 20) * TOP_K + jnp.arange(TOP_K)[None, :]
    slot_order = jnp.argsort(scores, axis=1)
    return jnp.take_along_axis(ordered, slot_order, axis=1).astype(jnp.int32)


def setup_inputs(seed: int = 0, part: int = 0) -> dict:
    base_key = jax.random.key(seed)
    key_x, key_route, key_gate = jax.random.split(jax.random.fold_in(base_key, part), 3)
    key_wg, key_wu, key_wd = jax.random.split(jax.random.key(seed + 1), 3)
    in_scale = D_MODEL ** -0.5
    out_scale = 2.0 * FFN_DIM ** -0.5
    tokens = jax.random.normal(key_x, (TOKENS, D_MODEL), jnp.float32).astype(jnp.bfloat16)
    expert_ids = draw_routing(key_route)
    logits = 1.5 * jax.random.normal(key_gate, (TOKENS, TOP_K), jnp.float32)
    gate_vals = jax.nn.softmax(logits, axis=-1)
    w_gate = (in_scale * jax.random.normal(key_wg, (NUM_EXPERTS, D_MODEL, FFN_DIM), jnp.float32)).astype(jnp.bfloat16)
    w_up = (in_scale * jax.random.normal(key_wu, (NUM_EXPERTS, D_MODEL, FFN_DIM), jnp.float32)).astype(jnp.bfloat16)
    w_down = (out_scale * jax.random.normal(key_wd, (NUM_EXPERTS, FFN_DIM, D_MODEL), jnp.float32)).astype(jnp.bfloat16)
    return {'tokens': tokens, 'expert_ids': expert_ids, 'gate_vals': gate_vals, 'w_gate': w_gate, 'w_up': w_up, 'w_down': w_down}


def expert_ffn(row_in, gate_mat, up_mat, down_mat):
    gate_act = jnp.dot(row_in, gate_mat, preferred_element_type=jnp.float32)
    up_act = jnp.dot(row_in, up_mat, preferred_element_type=jnp.float32)
    hidden = (jax.nn.silu(gate_act) * up_act).astype(jnp.bfloat16)
    return jnp.dot(hidden, down_mat, preferred_element_type=jnp.float32).astype(jnp.bfloat16)


def reference(tokens, expert_ids, gate_vals, w_gate, w_up, w_down):
    pair_count = TOKENS * TOP_K
    flat_ids = expert_ids.reshape(pair_count)
    pair_index = jnp.arange(pair_count, dtype=jnp.int32)

    def one_expert(map_item):
        expert, gate_mat, up_mat, down_mat = map_item
        member = flat_ids == expert
        slot_pos = jnp.where(member, jnp.cumsum(member.astype(jnp.int32)) - 1, EXPERT_CAP)
        pair_list = jnp.full((EXPERT_CAP,), pair_count, jnp.int32).at[slot_pos].set(pair_index, mode='drop')
        row_in = tokens[jnp.minimum(pair_list, pair_count - 1) // TOP_K]
        return pair_list, expert_ffn(row_in, gate_mat, up_mat, down_mat)

    pair_lists, expert_rows = lax.map(one_expert, (jnp.arange(NUM_EXPERTS, dtype=jnp.int32), w_gate, w_up, w_down))
    pair_out = jnp.zeros((pair_count, D_MODEL), jnp.bfloat16).at[pair_lists.reshape(-1)].set(expert_rows.reshape(-1, D_MODEL), mode='drop')
    earlier = jnp.arange(TOP_K)[None, :] < jnp.arange(TOP_K)[:, None]

    def combine_block(blk_item):
        rows_in, ids_in, gate_in, outs_in = blk_item
        dev_of = ids_in // LOCAL_EXPERTS
        same_dev = dev_of[:, :, None] == dev_of[:, None, :]
        weights = jnp.where(same_dev, gate_in[:, None, :], 0.0)
        dev_sum = jnp.einsum('tjk,tkd->tjd', weights, outs_in.astype(jnp.float32)).astype(jnp.bfloat16)
        leader = jnp.logical_not(jnp.any(same_dev & earlier[None, :, :], axis=2))
        moe_sum = jnp.sum(jnp.where(leader[:, :, None], dev_sum.astype(jnp.float32), 0.0), axis=1)
        return (rows_in.astype(jnp.float32) + moe_sum).astype(jnp.bfloat16)

    output = lax.map(combine_block, (tokens.reshape(GROUP, TOK_DEV, D_MODEL), expert_ids.reshape(GROUP, TOK_DEV, TOP_K), gate_vals.reshape(GROUP, TOK_DEV, TOP_K), pair_out.reshape(GROUP, TOK_DEV, TOP_K, D_MODEL)))
    return output.reshape(TOKENS, D_MODEL)
```

```python
import functools

import jax
import jax.numpy as jnp
from jax import lax
from jax.experimental import pallas as pl
from jax.experimental.pallas import tpu as pltpu
from jax.sharding import PartitionSpec as P

F32 = jnp.float32
BF16 = jnp.bfloat16
COLS = 256


def moe_kernel(groups, pair_cap, parts, x_ref, ids_ref, gates_ref, wg_hbm, wu_hbm, wd_hbm, out_ref,
               send_n, send_a, send_b, recv_n, recv_a, recv_b, sum_n, sum_a, sum_b, ret_n, ret_a, ret_b,
               sgate, rgate, gcol_n, gcol_a, gcol_b, pick_t, wg_buf, wu_buf, wd_buf, hid, acc, total,
               w_sem, ds_sem, dr_sem, gs_sem, gr_sem, cs_sem, cr_sem):
    me = lax.axis_index('ep')
    dp = lax.axis_index('dp')
    half_n = groups // 2
    half = me // half_n
    mine = me % half_n
    tok, d_model = x_ref.shape
    local_count, _, ffn = wg_hbm.shape
    top_k = ids_ref.shape[1]
    part_a, part_b = parts
    rows = {'n': pair_cap, 'a': part_a, 'b': part_b}
    base = {'n': 0, 'a': 0, 'b': part_a}
    send = {'n': send_n, 'a': send_a, 'b': send_b}
    recv = {'n': recv_n, 'a': recv_a, 'b': recv_b}
    sums = {'n': sum_n, 'a': sum_a, 'b': sum_b}
    ret = {'n': ret_n, 'a': ret_a, 'b': ret_b}
    gcol = {'n': gcol_n, 'a': gcol_a, 'b': gcol_b}
    row_of = {'n': 0, 'a': 1, 'b': 2}

    def device(phase, slot):
        side = half if phase == 'n' else 1 - half
        return (dp, side * half_n + slot)

    def slot_of(k):
        return lax.rem(mine + k, half_n)

    def first(phase):
        return 1 if phase == 'n' else 0

    def w_copy(which, expert, slot):
        hbm, buf = ((wg_hbm, wg_buf), (wu_hbm, wu_buf), (wd_hbm, wd_buf))[which]
        return pltpu.make_async_copy(hbm.at[expert], buf.at[slot], w_sem.at[which, slot])

    barrier = pltpu.get_barrier_semaphore()
    for k in range(1, half_n):
        pl.semaphore_signal(barrier, inc=1, device_id=device('n', slot_of(k)), device_id_type=pl.DeviceIdType.MESH)
    for k in range(half_n):
        pl.semaphore_signal(barrier, inc=1, device_id=device('a', slot_of(k)), device_id_type=pl.DeviceIdType.MESH)

    for expert in range(2):
        for which in range(3):
            w_copy(which, expert, expert).start()

    ids_t = ids_ref[...].T
    slot_ids = (ids_t + half * (half_n * local_count)) % (groups * local_count)
    slot_dev = slot_ids // local_count
    dev_iota = lax.broadcasted_iota(jnp.int32, (groups, tok), 0)
    chosen = dev_iota == slot_dev[0:1, :]
    for j in range(1, top_k):
        chosen = chosen | (dev_iota == slot_dev[j:j + 1, :])
    tri = (lax.broadcasted_iota(jnp.int32, (tok, tok), 0) <= lax.broadcasted_iota(jnp.int32, (tok, tok), 1)).astype(F32).astype(BF16)
    rank = jnp.dot(chosen.astype(F32).astype(BF16), tri, preferred_element_type=F32)
    rank = jnp.where(chosen, rank - 1.0, -1.0)

    def pick(phase):
        lo = 0 if phase == 'n' else half_n
        c_iota = lax.broadcasted_iota(jnp.int32, (half_n, rows[phase], tok), 1).astype(F32) + float(base[phase])
        mask = rank[lo:lo + half_n].reshape(half_n, 1, tok) == c_iota
        return mask.astype(F32).reshape(half_n * rows[phase], tok)

    def pack(phase):
        m = half_n * rows[phase]
        mat = pick(phase).astype(BF16)
        for n in range(0, d_model, COLS):
            part = jnp.dot(mat, x_ref[:, n:n + COLS], preferred_element_type=F32).astype(BF16)
            send[phase][:, :, n:n + COLS] = part.reshape(half_n, rows[phase], COLS)

    def row_copy(phase, slot):
        i = row_of[phase]
        return pltpu.make_async_remote_copy(
            src_ref=send[phase].at[slot], dst_ref=recv[phase].at[mine], send_sem=ds_sem.at[i, slot], recv_sem=dr_sem.at[i, mine],
            device_id=device(phase, slot), device_id_type=pl.DeviceIdType.MESH)

    def row_arrival(phase, slot):
        i = row_of[phase]
        return pltpu.make_async_remote_copy(
            src_ref=send[phase].at[slot], dst_ref=recv[phase].at[slot], send_sem=ds_sem.at[i, slot], recv_sem=dr_sem.at[i, slot],
            device_id=device(phase, slot), device_id_type=pl.DeviceIdType.MESH)

    def gate_copy(phase, slot, arrival=False):
        lo = 0 if phase == 'n' else half_n
        at = slot if arrival else mine
        return pltpu.make_async_remote_copy(
            src_ref=sgate.at[lo + slot], dst_ref=rgate.at[lo + at], send_sem=gs_sem.at[lo + slot], recv_sem=gr_sem.at[lo + at],
            device_id=device(phase, slot), device_id_type=pl.DeviceIdType.MESH)

    def sum_copy(phase, slot, arrival=False):
        i = row_of[phase]
        at = slot if arrival else mine
        return pltpu.make_async_remote_copy(
            src_ref=sums[phase].at[slot], dst_ref=ret[phase].at[at], send_sem=cs_sem.at[i, slot], recv_sem=cr_sem.at[i, at],
            device_id=device(phase, slot), device_id_type=pl.DeviceIdType.MESH)

    pack('n')
    pl.semaphore_wait(barrier, groups - 1)
    for k in range(1, half_n):
        row_copy('n', slot_of(k)).start()
    for phase in ('a', 'b'):
        pack(phase)
        for k in range(half_n):
            row_copy(phase, slot_of(k)).start()

    gates_t = gates_ref[...].T
    gd_row = lax.broadcasted_iota(jnp.int32, (groups * 8, tok), 0)
    gd_id = jnp.where(gd_row % 8 < local_count, (gd_row // 8) * local_count + gd_row % 8, -1)
    dense = jnp.zeros((groups * 8, tok), F32)
    for j in range(top_k):
        dense = dense + jnp.where(gd_id == slot_ids[j:j + 1, :], gates_t[j:j + 1, :], 0.0)
    lane_iota = lax.broadcasted_iota(jnp.int32, (128, tok), 0).astype(F32)
    for s in range(groups):
        mat = (rank[s:s + 1, :] == lane_iota).astype(F32)
        sgate[s] = lax.dot_general(dense[s * 8:(s + 1) * 8], mat, (((1,), (1,)), ((), ())),
                                   precision=lax.Precision.HIGHEST, preferred_element_type=F32)
    for k in range(1, half_n):
        gate_copy('n', slot_of(k)).start()
    for k in range(half_n):
        gate_copy('a', slot_of(k)).start()
    rgate[mine] = sgate[mine]
    recv_n[mine] = send_n[mine]

    col = 0
    cols_of = {}
    for phase in ('n', 'a', 'b'):
        m = half_n * rows[phase]
        pick_t[:, col:col + m] = pick(phase).T.astype(BF16)
        cols_of[phase] = (col, col + m)
        col += m

    def gate_columns(phase):
        lo = 0 if phase == 'n' else half_n
        for s in range(half_n):
            tile = rgate[lo + s].T
            gcol[phase][s * rows[phase]:(s + 1) * rows[phase], 0:8] = tile[base[phase]:base[phase] + rows[phase], :]

    def ffn_pass(phase, last):
        m = half_n * rows[phase]
        x_in = recv[phase]

        def step(expert, carry):
            slot = lax.rem(expert, 2)
            nxt = lax.rem(expert + 2, local_count)

            def refill(which):
                if last:
                    @pl.when(expert < local_count - 2)
                    def _():
                        w_copy(which, nxt, slot).start()
                else:
                    w_copy(which, nxt, slot).start()

            w_copy(0, expert, slot).wait()
            w_copy(1, expert, slot).wait()
            lhs = x_in[...].reshape(m, d_model)
            for n in range(0, ffn, COLS):
                w = min(COLS, ffn - n)
                g = jnp.dot(lhs, wg_buf[slot, :, n:n + w], preferred_element_type=F32)
                u = jnp.dot(lhs, wu_buf[slot, :, n:n + w], preferred_element_type=F32)
                hid[0:m, n:n + w] = (jax.nn.silu(g) * u).astype(BF16)
            refill(0)
            refill(1)
            w_copy(2, expert, slot).wait()
            gc = gcol[phase][...]
            g_col = jnp.sum(jnp.where(lax.broadcasted_iota(jnp.int32, gc.shape, 1) == expert, gc, 0.0), axis=1, keepdims=True)
            hv = hid[0:m, :]
            for n in range(0, d_model, COLS):
                y = jnp.dot(hv, wd_buf[slot, :, n:n + COLS], preferred_element_type=F32).astype(BF16).astype(F32)
                acc[0:m, n:n + COLS] = acc[0:m, n:n + COLS] + jnp.where(g_col > 0.0, g_col * y, 0.0)
            refill(2)
            return carry

        acc[0:m, :] = jnp.zeros((m, d_model), F32)
        lax.fori_loop(0, local_count, step, 0)
        sums[phase][...] = acc[0:m, :].astype(BF16).reshape(half_n, rows[phase], d_model)

    for phase in ('n', 'a', 'b'):
        for k in range(first(phase), half_n):
            row_arrival(phase, slot_of(k)).wait_recv()
            if phase != 'b':
                gate_copy(phase, slot_of(k), arrival=True).wait_recv()
        gate_columns(phase)
        ffn_pass(phase, phase == 'b')
        for k in range(first(phase), half_n):
            sum_copy(phase, slot_of(k)).start()
    ret_n[mine] = sum_n[mine]

    for phase in ('n', 'a', 'b'):
        for k in range(first(phase), half_n):
            sum_copy(phase, slot_of(k), arrival=True).wait_recv()
        m = half_n * rows[phase]
        lo, hi = cols_of[phase]
        got = ret[phase][...].reshape(m, d_model)
        pt = pick_t[:, lo:hi]
        for n in range(0, d_model, COLS):
            part = jnp.dot(pt, got[:, n:n + COLS], preferred_element_type=F32)
            if phase == 'n':
                total[:, n:n + COLS] = x_ref[:, n:n + COLS].astype(F32) + part
            elif phase == 'a':
                total[:, n:n + COLS] = total[:, n:n + COLS] + part
            else:
                out_ref[:, n:n + COLS] = (total[:, n:n + COLS] + part).astype(BF16)

    for phase in ('n', 'a', 'b'):
        for k in range(first(phase), half_n):
            row_copy(phase, slot_of(k)).wait_send()
            if phase != 'b':
                gate_copy(phase, slot_of(k)).wait_send()
            sum_copy(phase, slot_of(k)).wait_send()


def solution(mesh):
    groups = mesh.shape['ep']
    row_spec = P(('dp', 'ep'))
    expert_spec = P('ep')

    def device_step(tokens, expert_ids, gate_vals, w_gate, w_up, w_down):
        tok, top_k = expert_ids.shape
        d_model = tokens.shape[1]
        local_count, _, ffn = w_gate.shape
        pair_cap = tok * (top_k // 2) // groups
        part_b = (pair_cap // 3) // 16 * 16
        part_a = pair_cap - part_b
        half_n = groups // 2
        sizes = (pair_cap, part_a, part_b)

        def row_bufs():
            return [pltpu.VMEM((half_n, r, d_model), BF16) for r in sizes]

        scratch = row_bufs() + row_bufs() + row_bufs() + row_bufs() + [
            pltpu.VMEM((groups, 8, 128), F32),
            pltpu.VMEM((groups, 8, 128), F32),
        ] + [pltpu.VMEM((half_n * r, 8), F32) for r in sizes] + [
            pltpu.VMEM((tok, groups * pair_cap), BF16),
            pltpu.VMEM((2, d_model, ffn), BF16),
            pltpu.VMEM((2, d_model, ffn), BF16),
            pltpu.VMEM((2, ffn, d_model), BF16),
            pltpu.VMEM((half_n * pair_cap, ffn), BF16),
            pltpu.VMEM((half_n * pair_cap, d_model), F32),
            pltpu.VMEM((tok, d_model), F32),
            pltpu.SemaphoreType.DMA((3, 2)),
            pltpu.SemaphoreType.DMA((3, half_n)),
            pltpu.SemaphoreType.DMA((3, half_n)),
            pltpu.SemaphoreType.DMA((groups,)),
            pltpu.SemaphoreType.DMA((groups,)),
            pltpu.SemaphoreType.DMA((3, half_n)),
            pltpu.SemaphoreType.DMA((3, half_n)),
        ]
        vmem = pl.BlockSpec(memory_space=pltpu.VMEM)
        hbm = pl.BlockSpec(memory_space=pl.ANY)
        return pl.pallas_call(
            functools.partial(moe_kernel, groups, pair_cap, (part_a, part_b)),
            out_shape=jax.ShapeDtypeStruct((tok, d_model), BF16),
            in_specs=[vmem, vmem, vmem, hbm, hbm, hbm],
            out_specs=vmem,
            scratch_shapes=scratch,
            compiler_params=pltpu.CompilerParams(collective_id=0, has_side_effects=True, vmem_limit_bytes=66_000_000),
            name='moe_exchange',
        )(tokens, expert_ids, gate_vals, w_gate, w_up, w_down)

    return jax.shard_map(device_step, mesh=mesh, in_specs=(row_spec, row_spec, row_spec, expert_spec, expert_spec, expert_spec), out_specs=row_spec, check_vma=False)
```

```python
import functools

import jax
import jax.numpy as jnp
from jax import lax
from jax.experimental import pallas as pl
from jax.experimental.pallas import tpu as pltpu
from jax.sharding import PartitionSpec as P

F32 = jnp.float32
BF16 = jnp.bfloat16
COLS = 256
MESH_ID = pl.DeviceIdType.MESH


def moe_kernel(groups, pair_cap, x_ref, ids_ref, gates_ref, wg_hbm, wu_hbm, wd_hbm, out_ref,
               send, recv, sums, ret, sgate, rgate, gcol, pick_t, wg_buf, wu_buf, wd_buf, hid, acc, total,
               w_sem, ds_sem, dr_sem, gs_sem, gr_sem, cs_sem, cr_sem):
    me = lax.axis_index('ep')
    dp = lax.axis_index('dp')
    half_n = groups // 2
    quart = groups // 4
    half = me // half_n
    mine = me % half_n
    column = mine // quart
    tok, d_model = x_ref.shape
    local_count, _, ffn = wg_hbm.shape
    top_k = ids_ref.shape[0]
    m = quart * pair_cap
    base = {'y': quart * column, 'z': quart * (1 - column), 'a': half_n + quart * half, 'b': half_n + quart * (1 - half)}
    phases = ('y', 'b', 'z', 'a')

    def flip(k):
        slot, bit = 0, 1
        while bit < half_n:
            own = (mine // bit) % 2
            slot = slot + (1 - own if (k // bit) % 2 else own) * bit
            bit *= 2
        return slot

    near_y = [flip(k) for k in range(1, quart)]
    near_z = [flip(k) for k in range(quart, half_n)]
    far = [half_n + flip(k) for k in range(half_n)]
    members = {'y': near_y, 'z': near_z,
               'a': [base['a'] + flip(j) % quart for j in range(quart)], 'b': [base['b'] + flip(j) % quart for j in range(quart)]}

    def device(idx):
        side = idx // half_n
        return (dp, ((half + side) % 2) * half_n + idx % half_n)

    def own_at(idx):
        return (idx // half_n) * half_n + mine

    def w_copy(which, expert, slot):
        hbm, buf = ((wg_hbm, wg_buf), (wu_hbm, wu_buf), (wd_hbm, wd_buf))[which]
        return pltpu.make_async_copy(hbm.at[expert], buf.at[slot], w_sem.at[which, slot])

    def remote(src, dst, s_sem, r_sem, idx, arrival):
        at = idx if arrival else own_at(idx)
        return pltpu.make_async_remote_copy(
            src_ref=src.at[idx], dst_ref=dst.at[at], send_sem=s_sem.at[idx], recv_sem=r_sem.at[at],
            device_id=device(idx), device_id_type=MESH_ID)

    def row_copy(idx, arrival=False):
        return remote(send, recv, ds_sem, dr_sem, idx, arrival)

    def gate_copy(idx, arrival=False):
        return remote(sgate, rgate, gs_sem, gr_sem, idx, arrival)

    def sum_copy(idx, arrival=False):
        return remote(sums, ret, cs_sem, cr_sem, idx, arrival)

    barrier = pltpu.get_barrier_semaphore()
    others = near_y + near_z + far
    for idx in others:
        pl.semaphore_signal(barrier, inc=1, device_id=device(idx), device_id_type=MESH_ID)

    for expert in range(2):
        for which in range(3):
            w_copy(which, expert, expert).start()

    slot_ids = (ids_ref[...] + half * (half_n * local_count)) % (groups * local_count)
    slot_dev = slot_ids // local_count
    dev_iota = lax.broadcasted_iota(jnp.int32, (groups, tok), 0)
    chosen = dev_iota == slot_dev[0:1, :]
    for j in range(1, top_k):
        chosen = chosen | (dev_iota == slot_dev[j:j + 1, :])
    tri = (lax.broadcasted_iota(jnp.int32, (tok, tok), 0) <= lax.broadcasted_iota(jnp.int32, (tok, tok), 1)).astype(F32).astype(BF16)
    rank = jnp.dot(chosen.astype(F32).astype(BF16), tri, preferred_element_type=F32)
    rank = jnp.where(chosen, rank - 1.0, -1.0)

    def pick(lo, hi):
        c_iota = lax.broadcasted_iota(jnp.int32, (hi - lo, pair_cap, tok), 1).astype(F32)
        mask = rank[lo:hi].reshape(hi - lo, 1, tok) == c_iota
        return mask.astype(F32).reshape((hi - lo) * pair_cap, tok)

    def pack(lo, hi):
        mat = pick(lo, hi).astype(BF16)
        for n in range(0, d_model, COLS):
            part = jnp.dot(mat, x_ref[:, n:n + COLS], preferred_element_type=F32).astype(BF16)
            send[lo:hi, :, n:n + COLS] = part.reshape(hi - lo, pair_cap, COLS)

    pack(half_n, groups)
    pl.semaphore_wait(barrier, groups - 1)
    for idx in far[:quart]:
        row_copy(idx).start()
    pack(0, half_n)
    for idx in near_y:
        row_copy(idx).start()

    gd_row = lax.broadcasted_iota(jnp.int32, (groups * 8, tok), 0)
    gd_id = jnp.where(gd_row % 8 < local_count, (gd_row // 8) * local_count + gd_row % 8, -1)
    dense = jnp.zeros((groups * 8, tok), F32)
    for j in range(top_k):
        dense = dense + jnp.where(gd_id == slot_ids[j:j + 1, :], gates_ref[j:j + 1, :], 0.0)
    lane_iota = lax.broadcasted_iota(jnp.int32, (128, tok), 0).astype(F32)
    for s in range(groups):
        mat = (rank[s:s + 1, :] == lane_iota).astype(F32)
        sgate[s] = lax.dot_general(dense[s * 8:(s + 1) * 8], mat, (((1,), (1,)), ((), ())),
                                   precision=lax.Precision.HIGHEST, preferred_element_type=F32)
    for idx in far[:quart] + near_y:
        gate_copy(idx).start()
    for idx in far[quart:] + near_z:
        row_copy(idx).start()
        gate_copy(idx).start()
    rgate[mine] = sgate[mine]
    recv[mine] = send[mine]

    for s in range(0, groups, quart):
        pick_t[s // quart] = pick(s, s + quart).T.astype(BF16)

    def ffn_pass(phase, last):
        lo = base[phase]
        for j in range(quart):
            gcol[j * pair_cap:(j + 1) * pair_cap, :] = rgate[lo + j].T[0:pair_cap, :]

        def step(expert, carry):
            slot = lax.rem(expert, 2)
            nxt = lax.rem(expert + 2, local_count)

            def refill(which):
                if last:
                    @pl.when(expert < local_count - 2)
                    def _():
                        w_copy(which, nxt, slot).start()
                else:
                    w_copy(which, nxt, slot).start()

            w_copy(0, expert, slot).wait()
            w_copy(1, expert, slot).wait()
            lhs = recv[pl.ds(lo, quart)].reshape(m, d_model)
            for n in range(0, ffn, COLS):
                w = min(COLS, ffn - n)
                g = jnp.dot(lhs, wg_buf[slot, :, n:n + w], preferred_element_type=F32)
                u = jnp.dot(lhs, wu_buf[slot, :, n:n + w], preferred_element_type=F32)
                hid[:, n:n + w] = (jax.nn.silu(g) * u).astype(BF16)
            refill(0)
            refill(1)
            w_copy(2, expert, slot).wait()
            gc = gcol[...]
            g_col = jnp.sum(jnp.where(lax.broadcasted_iota(jnp.int32, gc.shape, 1) == expert, gc, 0.0), axis=1, keepdims=True)
            hv = hid[...]
            for n in range(0, d_model, COLS):
                y = jnp.dot(hv, wd_buf[slot, :, n:n + COLS], preferred_element_type=F32).astype(BF16).astype(F32)
                acc[:, n:n + COLS] = acc[:, n:n + COLS] + jnp.where(g_col > 0.0, g_col * y, 0.0)
            refill(2)
            return carry

        acc[...] = jnp.zeros((m, d_model), F32)
        lax.fori_loop(0, local_count, step, 0)
        sums[pl.ds(lo, quart)] = acc[...].astype(BF16).reshape(quart, pair_cap, d_model)

    for phase in phases:
        for idx in members[phase]:
            row_copy(idx, arrival=True).wait_recv()
            gate_copy(idx, arrival=True).wait_recv()
        ffn_pass(phase, phase == phases[-1])
        for idx in members[phase]:
            sum_copy(idx).start()
    ret[mine] = sums[mine]

    order = ('y', 'z', 'b', 'a')
    for phase in order:
        for idx in members[phase]:
            sum_copy(idx, arrival=True).wait_recv()
        lo = base[phase]
        got = ret[pl.ds(lo, quart)].reshape(m, d_model)
        pt = pick_t[lo // quart]
        for n in range(0, d_model, COLS):
            part = jnp.dot(pt, got[:, n:n + COLS], preferred_element_type=F32)
            if phase == order[0]:
                total[:, n:n + COLS] = x_ref[:, n:n + COLS].astype(F32) + part
            elif phase != order[-1]:
                total[:, n:n + COLS] = total[:, n:n + COLS] + part
            else:
                out_ref[:, n:n + COLS] = (total[:, n:n + COLS] + part).astype(BF16)

    for idx in others:
        row_copy(idx).wait_send()
        gate_copy(idx).wait_send()
        sum_copy(idx).wait_send()


def solution(mesh):
    groups = mesh.shape['ep']
    row_spec = P(('dp', 'ep'))
    expert_spec = P('ep')

    def device_step(tokens, expert_ids, gate_vals, w_gate, w_up, w_down):
        tok, top_k = expert_ids.shape
        d_model = tokens.shape[1]
        ffn = w_gate.shape[2]
        pair_cap = tok * (top_k // 2) // groups
        quart = groups // 4
        m = quart * pair_cap
        scratch = [pltpu.VMEM((groups, pair_cap, d_model), BF16) for _ in range(4)] + [
            pltpu.VMEM((groups, 8, 128), F32),
            pltpu.VMEM((groups, 8, 128), F32),
            pltpu.VMEM((m, 8), F32),
            pltpu.VMEM((4, tok, m), BF16),
            pltpu.VMEM((2, d_model, ffn), BF16),
            pltpu.VMEM((2, d_model, ffn), BF16),
            pltpu.VMEM((2, ffn, d_model), BF16),
            pltpu.VMEM((m, ffn), BF16),
            pltpu.VMEM((m, d_model), F32),
            pltpu.VMEM((tok, d_model), F32),
            pltpu.SemaphoreType.DMA((3, 2)),
        ] + [pltpu.SemaphoreType.DMA((groups,)) for _ in range(6)]
        vmem = pl.BlockSpec(memory_space=pltpu.VMEM)
        hbm = pl.BlockSpec(memory_space=pl.ANY)
        return pl.pallas_call(
            functools.partial(moe_kernel, groups, pair_cap),
            out_shape=jax.ShapeDtypeStruct((tok, d_model), BF16),
            in_specs=[vmem, vmem, vmem, hbm, hbm, hbm],
            out_specs=vmem,
            scratch_shapes=scratch,
            compiler_params=pltpu.CompilerParams(collective_id=0, has_side_effects=True, vmem_limit_bytes=66_000_000),
            name='moe_exchange',
        )(tokens, expert_ids.T, gate_vals.T, w_gate, w_up, w_down)

    return jax.shard_map(device_step, mesh=mesh, in_specs=(row_spec, row_spec, row_spec, expert_spec, expert_spec, expert_spec), out_specs=row_spec, check_vma=False)
```

```python
import functools

import jax
import jax.numpy as jnp
from jax import lax
from jax.experimental import pallas as pl
from jax.experimental.pallas import tpu as pltpu
from jax.sharding import PartitionSpec as P

F32 = jnp.float32
BF16 = jnp.bfloat16
COLS = 256
MESH_ID = pl.DeviceIdType.MESH


def moe_kernel(groups, pair_cap, x_ref, ids_ref, gates_ref, wg_hbm, wu_hbm, wd_hbm, out_ref,
               send, recv, sums, ret, sgate, rgate, gcol, pick_t, wg_buf, wu_buf, wd_buf, hid, acc, total,
               rank_out, rel_rank, rel_x, rel_send, w_sem, ds_sem, dr_sem, gs_sem, gr_sem, cs_sem, cr_sem, rel_ds, rel_s, rel_r):
    me = lax.axis_index('ep')
    dp = lax.axis_index('dp')
    half_n = groups // 2
    quart = groups // 4
    half = me // half_n
    mine = me % half_n
    column = mine // quart
    tok, d_model = x_ref.shape
    local_count, _, ffn = wg_hbm.shape
    top_k = ids_ref.shape[0]
    m = quart * pair_cap
    base = {'y': quart * column, 'z': quart * (1 - column), 'f': half_n + quart * column, 'g': half_n + quart * (1 - column)}
    phases = ('y', 'f', 'z', 'g')
    inner = (half + column) % 2

    def flip(k):
        slot, bit = 0, 1
        while bit < half_n:
            own = (mine // bit) % 2
            slot = slot + (1 - own if (k // bit) % 2 else own) * bit
            bit *= 2
        return slot

    near_y = [flip(k) for k in range(1, quart)]
    near_z = [flip(k) for k in range(quart, half_n)]
    far = [half_n + flip(k) for k in range(half_n)]
    members = {'y': near_y, 'z': near_z, 'f': far[:quart], 'g': far[quart:]}
    relayed = half_n + mine

    def device(idx):
        side = idx // half_n
        return (dp, ((half + side) % 2) * half_n + idx % half_n)

    def own_at(idx):
        return (idx // half_n) * half_n + mine

    def w_copy(which, expert, slot):
        hbm, buf = ((wg_hbm, wg_buf), (wu_hbm, wu_buf), (wd_hbm, wd_buf))[which]
        return pltpu.make_async_copy(hbm.at[expert], buf.at[slot], w_sem.at[which, slot])

    def remote(src, dst, s_sem, r_sem, idx, arrival):
        at = idx if arrival else own_at(idx)
        return pltpu.make_async_remote_copy(
            src_ref=src.at[idx], dst_ref=dst.at[at], send_sem=s_sem.at[idx], recv_sem=r_sem.at[at],
            device_id=device(idx), device_id_type=MESH_ID)

    def row_copy(idx, arrival=False):
        return remote(send, recv, ds_sem, dr_sem, idx, arrival)

    def relay_copy(slot):
        return pltpu.make_async_remote_copy(
            src_ref=rel_send.at[slot], dst_ref=recv.at[relayed], send_sem=rel_ds.at[slot], recv_sem=dr_sem.at[relayed],
            device_id=device(slot), device_id_type=MESH_ID)

    def relay_in(which):
        src, dst = ((x_ref, rel_x), (rank_out, rel_rank))[which]
        return pltpu.make_async_remote_copy(
            src_ref=src, dst_ref=dst, send_sem=rel_s.at[which], recv_sem=rel_r.at[which],
            device_id=device(relayed), device_id_type=MESH_ID)

    def gate_copy(idx, arrival=False):
        return remote(sgate, rgate, gs_sem, gr_sem, idx, arrival)

    def sum_copy(idx, arrival=False):
        return remote(sums, ret, cs_sem, cr_sem, idx, arrival)

    barrier = pltpu.get_barrier_semaphore()
    others = near_y + near_z + far
    for idx in others:
        pl.semaphore_signal(barrier, inc=1, device_id=device(idx), device_id_type=MESH_ID)

    for expert in range(2):
        for which in range(3):
            w_copy(which, expert, expert).start()

    slot_ids = (ids_ref[...] + half * (half_n * local_count)) % (groups * local_count)
    slot_dev = slot_ids // local_count
    dev_iota = lax.broadcasted_iota(jnp.int32, (groups, tok), 0)
    chosen = dev_iota == slot_dev[0:1, :]
    for j in range(1, top_k):
        chosen = chosen | (dev_iota == slot_dev[j:j + 1, :])
    tri = (lax.broadcasted_iota(jnp.int32, (tok, tok), 0) <= lax.broadcasted_iota(jnp.int32, (tok, tok), 1)).astype(F32).astype(BF16)
    rank = jnp.dot(chosen.astype(F32).astype(BF16), tri, preferred_element_type=F32)
    rank = jnp.where(chosen, rank - 1.0, -1.0)

    rank_out[...] = rank[half_n:groups]

    def pick(ranks):
        n = ranks.shape[0]
        c_iota = lax.broadcasted_iota(jnp.int32, (n, pair_cap, tok), 1).astype(F32)
        mask = ranks.reshape(n, 1, tok) == c_iota
        return mask.astype(F32).reshape(n * pair_cap, tok)

    def pack(ranks, src, dst, lo):
        n_part = ranks.shape[0]
        mat = pick(ranks).astype(BF16)
        for n in range(0, d_model, COLS):
            part = jnp.dot(mat, src[:, n:n + COLS], preferred_element_type=F32).astype(BF16)
            dst[lo:lo + n_part, :, n:n + COLS] = part.reshape(n_part, pair_cap, COLS)

    pl.semaphore_wait(barrier, groups - 1)

    @pl.when(inner == 0)
    def _():
        relay_in(1).start()
        relay_in(0).start()

    @pl.when(inner == 1)
    def _():
        pack(rank[half_n:groups], x_ref, send, half_n)
        for idx in far[:quart]:
            row_copy(idx).start()

    pack(rank[0:half_n], x_ref, send, 0)
    for idx in near_y:
        row_copy(idx).start()

    gd_row = lax.broadcasted_iota(jnp.int32, (groups * 8, tok), 0)
    gd_id = jnp.where(gd_row % 8 < local_count, (gd_row // 8) * local_count + gd_row % 8, -1)
    dense = jnp.zeros((groups * 8, tok), F32)
    for j in range(top_k):
        dense = dense + jnp.where(gd_id == slot_ids[j:j + 1, :], gates_ref[j:j + 1, :], 0.0)
    lane_iota = lax.broadcasted_iota(jnp.int32, (128, tok), 0).astype(F32)
    for s in range(groups):
        mat = (rank[s:s + 1, :] == lane_iota).astype(F32)
        sgate[s] = lax.dot_general(dense[s * 8:(s + 1) * 8], mat, (((1,), (1,)), ((), ())),
                                   precision=lax.Precision.HIGHEST, preferred_element_type=F32)
    for idx in others:
        gate_copy(idx).start()
    for idx in near_z:
        row_copy(idx).start()

    @pl.when(inner == 1)
    def _():
        for idx in far[quart:]:
            row_copy(idx).start()

    rgate[mine] = sgate[mine]
    recv[mine] = send[mine]

    for s in range(0, groups, quart):
        pick_t[s // quart] = pick(rank[s:s + quart]).T.astype(BF16)

    def relay():
        relay_in(1).wait_recv()
        relay_in(0).wait_recv()
        pack(rel_rank[...], rel_x, rel_send, 0)
        for slot in near_z + near_y:
            relay_copy(slot).start()
        recv[relayed] = rel_send[mine]

    def ffn_pass(phase):
        lo = base[phase]
        turn = phases.index(phase)
        for j in range(quart):
            gcol[j * pair_cap:(j + 1) * pair_cap, :] = rgate[lo + j].T[0:pair_cap, :]

        def step(i, carry):
            expert = i if turn % 2 == 0 else local_count - 1 - i
            nxt = expert + 2 if turn % 2 == 0 else expert - 2
            slot = lax.rem(expert, 2)

            def refill(which):
                @pl.when(i < local_count - 2)
                def _():
                    w_copy(which, nxt, slot).start()

            def arrive(which):
                if turn == 0:
                    w_copy(which, expert, slot).wait()
                else:
                    @pl.when(i >= 2)
                    def _():
                        w_copy(which, expert, slot).wait()

            arrive(0)
            arrive(1)
            lhs = recv[pl.ds(lo, quart)].reshape(m, d_model)
            for n in range(0, ffn, COLS):
                w = min(COLS, ffn - n)
                g = jnp.dot(lhs, wg_buf[slot, :, n:n + w], preferred_element_type=F32)
                u = jnp.dot(lhs, wu_buf[slot, :, n:n + w], preferred_element_type=F32)
                hid[:, n:n + w] = (jax.nn.silu(g) * u).astype(BF16)
            refill(0)
            refill(1)
            arrive(2)
            gc = gcol[...]
            g_col = jnp.sum(jnp.where(lax.broadcasted_iota(jnp.int32, gc.shape, 1) == expert, gc, 0.0), axis=1, keepdims=True)
            hv = hid[...]
            for n in range(0, d_model, COLS):
                y = jnp.dot(hv, wd_buf[slot, :, n:n + COLS], preferred_element_type=F32).astype(BF16).astype(F32)
                acc[:, n:n + COLS] = acc[:, n:n + COLS] + jnp.where(g_col > 0.0, g_col * y, 0.0)
            refill(2)
            return carry

        acc[...] = jnp.zeros((m, d_model), F32)
        lax.fori_loop(0, local_count, step, 0)
        sums[pl.ds(lo, quart)] = acc[...].astype(BF16).reshape(quart, pair_cap, d_model)

    for phase in phases:
        if phase == 'y':
            pl.when(inner == 1)(relay)
        for idx in members[phase]:
            gate_copy(idx, arrival=True).wait_recv()
            if phase == 'f' and idx is members[phase][0]:
                pl.when(inner == 0)(lambda idx=idx: row_copy(idx, arrival=True).wait_recv())
            else:
                row_copy(idx, arrival=True).wait_recv()
        ffn_pass(phase)
        for idx in members[phase]:
            sum_copy(idx).start()
    ret[mine] = sums[mine]

    order = ('y', 'z', 'f', 'g')
    for phase in order:
        for idx in members[phase]:
            sum_copy(idx, arrival=True).wait_recv()
        lo = base[phase]
        got = ret[pl.ds(lo, quart)].reshape(m, d_model)
        pt = pick_t[lo // quart]
        for n in range(0, d_model, COLS):
            part = jnp.dot(pt, got[:, n:n + COLS], preferred_element_type=F32)
            if phase == order[0]:
                total[:, n:n + COLS] = x_ref[:, n:n + COLS].astype(F32) + part
            elif phase != order[-1]:
                total[:, n:n + COLS] = total[:, n:n + COLS] + part
            else:
                out_ref[:, n:n + COLS] = (total[:, n:n + COLS] + part).astype(BF16)

    for idx in others:
        gate_copy(idx).wait_send()
        sum_copy(idx).wait_send()
    for idx in near_y + near_z:
        row_copy(idx).wait_send()

    @pl.when(inner == 0)
    def _():
        relay_in(1).wait_send()
        relay_in(0).wait_send()

    @pl.when(inner == 1)
    def _():
        for idx in far:
            row_copy(idx).wait_send()
        for slot in near_z + near_y:
            relay_copy(slot).wait_send()


def solution(mesh):
    groups = mesh.shape['ep']
    row_spec = P(('dp', 'ep'))
    expert_spec = P('ep')

    def device_step(tokens, expert_ids, gate_vals, w_gate, w_up, w_down):
        tok, top_k = expert_ids.shape
        d_model = tokens.shape[1]
        ffn = w_gate.shape[2]
        pair_cap = tok * (top_k // 2) // groups
        quart = groups // 4
        m = quart * pair_cap
        scratch = [pltpu.VMEM((groups, pair_cap, d_model), BF16) for _ in range(4)] + [
            pltpu.VMEM((groups, 8, 128), F32),
            pltpu.VMEM((groups, 8, 128), F32),
            pltpu.VMEM((m, 8), F32),
            pltpu.VMEM((4, tok, m), BF16),
            pltpu.VMEM((2, d_model, ffn), BF16),
            pltpu.VMEM((2, d_model, ffn), BF16),
            pltpu.VMEM((2, ffn, d_model), BF16),
            pltpu.VMEM((m, ffn), BF16),
            pltpu.VMEM((m, d_model), F32),
            pltpu.VMEM((tok, d_model), F32),
            pltpu.VMEM((groups // 2, tok), F32),
            pltpu.VMEM((groups // 2, tok), F32),
            pltpu.VMEM((tok, d_model), BF16),
            pltpu.VMEM((groups // 2, pair_cap, d_model), BF16),
            pltpu.SemaphoreType.DMA((3, 2)),
        ] + [pltpu.SemaphoreType.DMA((groups,)) for _ in range(6)] + [pltpu.SemaphoreType.DMA((groups // 2,)), pltpu.SemaphoreType.DMA((2,)), pltpu.SemaphoreType.DMA((2,))]
        vmem = pl.BlockSpec(memory_space=pltpu.VMEM)
        hbm = pl.BlockSpec(memory_space=pl.ANY)
        return pl.pallas_call(
            functools.partial(moe_kernel, groups, pair_cap),
            out_shape=jax.ShapeDtypeStruct((tok, d_model), BF16),
            in_specs=[vmem, vmem, vmem, hbm, hbm, hbm],
            out_specs=vmem,
            scratch_shapes=scratch,
            compiler_params=pltpu.CompilerParams(collective_id=0, has_side_effects=True, vmem_limit_bytes=66_000_000),
            name='moe_exchange',
        )(tokens, expert_ids.T, gate_vals.T, w_gate, w_up, w_down)

    return jax.shard_map(device_step, mesh=mesh, in_specs=(row_spec, row_spec, row_spec, expert_spec, expert_spec, expert_spec), out_specs=row_spec, check_vma=False)
```

```python
import functools

import jax
import jax.numpy as jnp
from jax import lax
from jax.experimental import pallas as pl
from jax.experimental.pallas import tpu as pltpu
from jax.sharding import PartitionSpec as P

F32 = jnp.float32
BF16 = jnp.bfloat16
COLS = 256
MESH_ID = pl.DeviceIdType.MESH


def moe_kernel(groups, pair_cap, x_ref, ids_ref, gates_ref, wg_hbm, wu_hbm, wd_hbm, out_ref,
               send, recv, sums, ret, sgate, rgate, gcol, pick_t, wg_buf, wu_buf, wd_buf, hid, acc, total,
               rank_out, rel_rank, rel_x, rel_send, w_sem, ds_sem, dr_sem, gs_sem, gr_sem, cs_sem, cr_sem, rel_ds, rel_s, rel_r, go_sem):
    me = lax.axis_index('ep')
    dp = lax.axis_index('dp')
    half_n = groups // 2
    quart = groups // 4
    half = me // half_n
    mine = me % half_n
    column = mine // quart
    tok, d_model = x_ref.shape
    local_count, _, ffn = wg_hbm.shape
    top_k = ids_ref.shape[0]
    m = quart * pair_cap
    base = {'y': quart * column, 'z': quart * (1 - column), 'f': half_n + quart * half, 'g': half_n + quart * (1 - half)}
    inner = (half + column) % 2

    def flip(k):
        slot, bit = 0, 1
        while bit < half_n:
            own = (mine // bit) % 2
            slot = slot + (1 - own if (k // bit) % 2 else own) * bit
            bit *= 2
        return slot

    near_y = [flip(k) for k in range(1, quart)]
    near_z = [flip(k) for k in range(quart, half_n)]
    far = [half_n + flip(k) for k in range(half_n)]
    members = {'y': near_y, 'z': near_z, 'f': [base['f'] + flip(k) % quart for k in range(quart)],
               'g': [base['g'] + flip(k) % quart for k in range(quart)]}

    def either(a, b):
        return inner * a + (1 - inner) * b

    base.update(p=either(base['f'], base['z']), q=either(base['z'], base['f']))
    members.update(p=[either(a, b) for a, b in zip(members['f'], members['z'])],
                   q=[either(b, a) for a, b in zip(members['f'], members['z'])])
    phases = ('p', 'q', 'g', 'y')
    relayed = (members['f'][0], members['g'][0])

    def device(idx):
        side = idx // half_n
        return (dp, ((half + side) % 2) * half_n + idx % half_n)

    def own_at(idx):
        return (idx // half_n) * half_n + mine

    def w_copy(which, expert, slot):
        hbm, buf = ((wg_hbm, wg_buf), (wu_hbm, wu_buf), (wd_hbm, wd_buf))[which]
        return pltpu.make_async_copy(hbm.at[expert], buf.at[slot], w_sem.at[which, slot])

    def remote(src, dst, s_sem, r_sem, idx, arrival):
        at = idx if arrival else own_at(idx)
        return pltpu.make_async_remote_copy(
            src_ref=src.at[idx], dst_ref=dst.at[at], send_sem=s_sem.at[idx], recv_sem=r_sem.at[at],
            device_id=device(idx), device_id_type=MESH_ID)

    def row_copy(idx, arrival=False):
        return remote(send, recv, ds_sem, dr_sem, idx, arrival)

    def relay_copy(which, slot):
        src, at = ((rel_send, slot), (send, half_n + slot))[which]
        return pltpu.make_async_remote_copy(
            src_ref=src.at[at], dst_ref=recv.at[relayed[which]], send_sem=rel_ds.at[which, slot], recv_sem=dr_sem.at[relayed[which]],
            device_id=device(slot), device_id_type=MESH_ID)

    def relay_in(kind, slot):
        src, dst = ((x_ref, rel_x), (rank_out, rel_rank))[kind]
        return pltpu.make_async_remote_copy(
            src_ref=src, dst_ref=dst.at[slot], send_sem=rel_s.at[kind], recv_sem=rel_r.at[kind, slot],
            device_id=device(members['f'][0]), device_id_type=MESH_ID)

    def gate_copy(idx, arrival=False):
        return remote(sgate, rgate, gs_sem, gr_sem, idx, arrival)

    def sum_copy(idx, arrival=False):
        return remote(sums, ret, cs_sem, cr_sem, idx, arrival)

    barrier = pltpu.get_barrier_semaphore()
    others = near_y + near_z + far
    for idx in others:
        pl.semaphore_signal(barrier, inc=1, device_id=device(idx), device_id_type=MESH_ID)

    for expert in range(2):
        for which in range(3):
            w_copy(which, expert, expert).start()

    slot_ids = (ids_ref[...] + half * (half_n * local_count)) % (groups * local_count)
    slot_dev = slot_ids // local_count
    dev_iota = lax.broadcasted_iota(jnp.int32, (groups, tok), 0)
    chosen = dev_iota == slot_dev[0:1, :]
    for j in range(1, top_k):
        chosen = chosen | (dev_iota == slot_dev[j:j + 1, :])
    tri = (lax.broadcasted_iota(jnp.int32, (tok, tok), 0) <= lax.broadcasted_iota(jnp.int32, (tok, tok), 1)).astype(F32).astype(BF16)
    rank = jnp.dot(chosen.astype(F32).astype(BF16), tri, preferred_element_type=F32)
    rank = jnp.where(chosen, rank - 1.0, -1.0)

    rank_out[...] = rank[half_n:groups]

    def pick(ranks):
        n = ranks.shape[0]
        c_iota = lax.broadcasted_iota(jnp.int32, (n, pair_cap, tok), 1).astype(F32)
        mask = ranks.reshape(n, 1, tok) == c_iota
        return mask.astype(F32).reshape(n * pair_cap, tok)

    def pack(ranks, src, dst, lo):
        n_part = ranks.shape[0]
        mat = pick(ranks).astype(BF16)
        for n in range(0, d_model, COLS):
            part = jnp.dot(mat, src[:, n:n + COLS], preferred_element_type=F32).astype(BF16)
            dst[lo:lo + n_part, :, n:n + COLS] = part.reshape(n_part, pair_cap, COLS)

    pl.semaphore_wait(barrier, groups - 1)

    @pl.when(inner == 1)
    def _():
        relay_in(1, 0).start()
        relay_in(0, 0).start()

    pack(rank[0:half_n], x_ref, send, 0)
    for idx in near_z + near_y:
        row_copy(idx).start()

    gd_row = lax.broadcasted_iota(jnp.int32, (groups * 8, tok), 0)
    gd_id = jnp.where(gd_row % 8 < local_count, (gd_row // 8) * local_count + gd_row % 8, -1)
    dense = jnp.zeros((groups * 8, tok), F32)
    for j in range(top_k):
        dense = dense + jnp.where(gd_id == slot_ids[j:j + 1, :], gates_ref[j:j + 1, :], 0.0)
    lane_iota = lax.broadcasted_iota(jnp.int32, (128, tok), 0).astype(F32)
    for s in range(groups):
        mat = (rank[s:s + 1, :] == lane_iota).astype(F32)
        sgate[s] = lax.dot_general(dense[s * 8:(s + 1) * 8], mat, (((1,), (1,)), ((), ())),
                                   precision=lax.Precision.HIGHEST, preferred_element_type=F32)
    for idx in far + near_z + near_y:
        gate_copy(idx).start()
    rgate[mine] = sgate[mine]
    recv[mine] = send[mine]

    for s in range(0, groups, quart):
        pick_t[s // quart] = pick(rank[s:s + quart]).T.astype(BF16)

    def relay(which):
        relay_in(1, which).wait_recv()
        relay_in(0, which).wait_recv()
        buf, lo = ((rel_send, 0), (send, half_n))[which]
        pack(rel_rank[which], rel_x.at[which], buf, lo)
        for slot in near_y + near_z:
            relay_copy(which, slot).start()
        recv[relayed[which]] = buf[lo + mine]

    @pl.when(inner == 1)
    def _():
        relay_in(1, 0).wait_send()
        relay_in(0, 0).wait_send()
        for idx in far:
            gate_copy(idx).wait_send()
        pl.semaphore_signal(go_sem, inc=1, device_id=device(near_z[0]), device_id_type=MESH_ID)
        relay(0)

    @pl.when(inner == 0)
    def _():
        for idx in far:
            gate_copy(idx).wait_send()
        pl.semaphore_wait(go_sem, 1)
        relay_in(1, 1).start()
        relay_in(0, 1).start()

    def ffn_pass(phase):
        lo = base[phase]
        turn = phases.index(phase)
        for j in range(quart):
            gcol[j * pair_cap:(j + 1) * pair_cap, :] = rgate[lo + j].T[0:pair_cap, :]

        def step(i, carry):
            expert = i if turn % 2 == 0 else local_count - 1 - i
            nxt = expert + 2 if turn % 2 == 0 else expert - 2
            slot = lax.rem(expert, 2)

            def refill(which):
                @pl.when(i < local_count - 2)
                def _():
                    w_copy(which, nxt, slot).start()

            def arrive(which):
                if turn == 0:
                    w_copy(which, expert, slot).wait()
                else:
                    @pl.when(i >= 2)
                    def _():
                        w_copy(which, expert, slot).wait()

            arrive(0)
            arrive(1)
            lhs = recv[pl.ds(lo, quart)].reshape(m, d_model)
            for n in range(0, ffn, COLS):
                w = min(COLS, ffn - n)
                g = jnp.dot(lhs, wg_buf[slot, :, n:n + w], preferred_element_type=F32)
                u = jnp.dot(lhs, wu_buf[slot, :, n:n + w], preferred_element_type=F32)
                hid[:, n:n + w] = (jax.nn.silu(g) * u).astype(BF16)
            refill(0)
            refill(1)
            arrive(2)
            gc = gcol[...]
            g_col = jnp.sum(jnp.where(lax.broadcasted_iota(jnp.int32, gc.shape, 1) == expert, gc, 0.0), axis=1, keepdims=True)
            hv = hid[...]
            for n in range(0, d_model, COLS):
                y = jnp.dot(hv, wd_buf[slot, :, n:n + COLS], preferred_element_type=F32).astype(BF16).astype(F32)
                acc[:, n:n + COLS] = acc[:, n:n + COLS] + jnp.where(g_col > 0.0, g_col * y, 0.0)
            refill(2)
            return carry

        acc[...] = jnp.zeros((m, d_model), F32)
        lax.fori_loop(0, local_count, step, 0)
        sums[pl.ds(lo, quart)] = acc[...].astype(BF16).reshape(quart, pair_cap, d_model)

    for phase in phases:
        if phase == 'q':
            pl.when(inner == 1)(lambda: relay(1))
        for idx in members[phase]:
            gate_copy(idx, arrival=True).wait_recv()
            if phase in ('p', 'g') and idx is members[phase][0]:
                pl.when(inner == 0)(lambda idx=idx: row_copy(idx, arrival=True).wait_recv())
            else:
                row_copy(idx, arrival=True).wait_recv()
        ffn_pass(phase)
        for idx in members[phase]:
            sum_copy(idx).start()
    ret[mine] = sums[mine]

    order = ('z', 'y', 'g', 'f')
    for phase in order:
        for idx in members[phase]:
            sum_copy(idx, arrival=True).wait_recv()
        lo = base[phase]
        got = ret[pl.ds(lo, quart)].reshape(m, d_model)
        pt = pick_t[lo // quart]
        for n in range(0, d_model, COLS):
            part = jnp.dot(pt, got[:, n:n + COLS], preferred_element_type=F32)
            if phase == order[0]:
                total[:, n:n + COLS] = x_ref[:, n:n + COLS].astype(F32) + part
            elif phase != order[-1]:
                total[:, n:n + COLS] = total[:, n:n + COLS] + part
            else:
                out_ref[:, n:n + COLS] = (total[:, n:n + COLS] + part).astype(BF16)

    for idx in others:
        sum_copy(idx).wait_send()
    for idx in near_y + near_z:
        row_copy(idx).wait_send()
        gate_copy(idx).wait_send()

    @pl.when(inner == 0)
    def _():
        relay_in(1, 1).wait_send()
        relay_in(0, 1).wait_send()

    @pl.when(inner == 1)
    def _():
        for slot in near_z + near_y:
            relay_copy(0, slot).wait_send()
            relay_copy(1, slot).wait_send()


def solution(mesh):
    groups = mesh.shape['ep']
    row_spec = P(('dp', 'ep'))
    expert_spec = P('ep')

    def device_step(tokens, expert_ids, gate_vals, w_gate, w_up, w_down):
        tok, top_k = expert_ids.shape
        d_model = tokens.shape[1]
        ffn = w_gate.shape[2]
        pair_cap = tok * (top_k // 2) // groups
        quart = groups // 4
        m = quart * pair_cap
        scratch = [pltpu.VMEM((groups, pair_cap, d_model), BF16) for _ in range(4)] + [
            pltpu.VMEM((groups, 8, 128), F32),
            pltpu.VMEM((groups, 8, 128), F32),
            pltpu.VMEM((m, 8), F32),
            pltpu.VMEM((4, tok, m), BF16),
            pltpu.VMEM((2, d_model, ffn), BF16),
            pltpu.VMEM((2, d_model, ffn), BF16),
            pltpu.VMEM((2, ffn, d_model), BF16),
            pltpu.VMEM((m, ffn), BF16),
            pltpu.VMEM((m, d_model), F32),
            pltpu.VMEM((tok, d_model), F32),
            pltpu.VMEM((groups // 2, tok), F32),
            pltpu.VMEM((2, groups // 2, tok), F32),
            pltpu.VMEM((2, tok, d_model), BF16),
            pltpu.VMEM((groups // 2, pair_cap, d_model), BF16),
            pltpu.SemaphoreType.DMA((3, 2)),
        ] + [pltpu.SemaphoreType.DMA((groups,)) for _ in range(6)] + [
            pltpu.SemaphoreType.DMA((2, groups // 2)), pltpu.SemaphoreType.DMA((2,)), pltpu.SemaphoreType.DMA((2, 2)), pltpu.SemaphoreType.REGULAR]
        vmem = pl.BlockSpec(memory_space=pltpu.VMEM)
        hbm = pl.BlockSpec(memory_space=pl.ANY)
        return pl.pallas_call(
            functools.partial(moe_kernel, groups, pair_cap),
            out_shape=jax.ShapeDtypeStruct((tok, d_model), BF16),
            in_specs=[vmem, vmem, vmem, hbm, hbm, hbm],
            out_specs=vmem,
            scratch_shapes=scratch,
            compiler_params=pltpu.CompilerParams(collective_id=0, has_side_effects=True, vmem_limit_bytes=66_000_000),
            name='moe_exchange',
        )(tokens, expert_ids.T, gate_vals.T, w_gate, w_up, w_down)

    return jax.shard_map(device_step, mesh=mesh, in_specs=(row_spec, row_spec, row_spec, expert_spec, expert_spec, expert_spec), out_specs=row_spec, check_vma=False)
```

```python
import functools

import jax
import jax.numpy as jnp
from jax import lax
from jax.experimental import pallas as pl
from jax.experimental.pallas import tpu as pltpu
from jax.sharding import PartitionSpec as P

F32 = jnp.float32
BF16 = jnp.bfloat16
COLS = 256
MESH_ID = pl.DeviceIdType.MESH


def moe_kernel(groups, pair_cap, x_ref, ids_ref, gates_ref, wg_hbm, wu_hbm, wd_hbm, out_ref,
               send, recv, sums, ret, sgate, rgate, gcol, pick_t, wg_buf, wu_buf, wd_buf, hid, acc, total,
               rank_out, rel_rank, rel_x, rel_send, w_sem, ds_sem, dr_sem, gs_sem, gr_sem, cs_sem, cr_sem, rel_ds, rel_s, rel_r, go_sem):
    me = lax.axis_index('ep')
    dp = lax.axis_index('dp')
    half_n = groups // 2
    quart = groups // 4
    half = me // half_n
    mine = me % half_n
    column = mine // quart
    tok, d_model = x_ref.shape
    local_count, _, ffn = wg_hbm.shape
    top_k = ids_ref.shape[0]
    m = quart * pair_cap
    base = {'y': quart * column, 'z': quart * (1 - column), 'f': half_n + quart * half, 'g': half_n + quart * (1 - half)}
    inner = (half + column) % 2

    def flip(k):
        slot, bit = 0, 1
        while bit < half_n:
            own = (mine // bit) % 2
            slot = slot + (1 - own if (k // bit) % 2 else own) * bit
            bit *= 2
        return slot

    near_y = [flip(k) for k in range(1, quart)]
    near_z = [flip(k) for k in range(quart, half_n)]
    far = [half_n + flip(k) for k in range(half_n)]
    members = {'y': near_y, 'z': near_z, 'f': [base['f'] + flip(k) % quart for k in range(quart)],
               'g': [base['g'] + flip(k) % quart for k in range(quart)]}

    def either(a, b):
        return inner * a + (1 - inner) * b

    base.update(p=either(base['f'], base['z']), q=either(base['z'], base['f']))
    members.update(p=[either(a, b) for a, b in zip(members['f'], members['z'])],
                   q=[either(b, a) for a, b in zip(members['f'], members['z'])])
    phases = ('p', 'q', 'g', 'y')
    relayed = (members['f'][0], members['g'][0])

    def device(idx):
        side = idx // half_n
        return (dp, ((half + side) % 2) * half_n + idx % half_n)

    def own_at(idx):
        return (idx // half_n) * half_n + mine

    def w_copy(which, expert, slot):
        hbm, buf = ((wg_hbm, wg_buf), (wu_hbm, wu_buf), (wd_hbm, wd_buf))[which]
        return pltpu.make_async_copy(hbm.at[expert], buf.at[slot], w_sem.at[which, slot])

    def remote(src, dst, s_sem, r_sem, idx, arrival):
        at = idx if arrival else own_at(idx)
        return pltpu.make_async_remote_copy(
            src_ref=src.at[idx], dst_ref=dst.at[at], send_sem=s_sem.at[idx], recv_sem=r_sem.at[at],
            device_id=device(idx), device_id_type=MESH_ID)

    def row_copy(idx, arrival=False):
        return remote(send, recv, ds_sem, dr_sem, idx, arrival)

    def relay_copy(which, slot):
        src, at = ((rel_send, slot), (send, half_n + slot))[which]
        return pltpu.make_async_remote_copy(
            src_ref=src.at[at], dst_ref=recv.at[relayed[which]], send_sem=rel_ds.at[which, slot], recv_sem=dr_sem.at[relayed[which]],
            device_id=device(slot), device_id_type=MESH_ID)

    def relay_in(kind, slot):
        src, dst = ((x_ref, rel_x), (rank_out, rel_rank))[kind]
        return pltpu.make_async_remote_copy(
            src_ref=src, dst_ref=dst.at[slot], send_sem=rel_s.at[kind], recv_sem=rel_r.at[kind, slot],
            device_id=device(members['f'][0]), device_id_type=MESH_ID)

    def gate_copy(idx, arrival=False):
        return remote(sgate, rgate, gs_sem, gr_sem, idx, arrival)

    def sum_copy(idx, arrival=False):
        return remote(sums, ret, cs_sem, cr_sem, idx, arrival)

    barrier = pltpu.get_barrier_semaphore()
    others = near_y + near_z + far
    for idx in others:
        pl.semaphore_signal(barrier, inc=1, device_id=device(idx), device_id_type=MESH_ID)

    for expert in range(2):
        for which in range(3):
            w_copy(which, expert, expert).start()

    slot_ids = (ids_ref[...] + half * (half_n * local_count)) % (groups * local_count)
    slot_dev = slot_ids // local_count
    dev_iota = lax.broadcasted_iota(jnp.int32, (groups, tok), 0)
    chosen = dev_iota == slot_dev[0:1, :]
    for j in range(1, top_k):
        chosen = chosen | (dev_iota == slot_dev[j:j + 1, :])
    tri = (lax.broadcasted_iota(jnp.int32, (tok, tok), 0) <= lax.broadcasted_iota(jnp.int32, (tok, tok), 1)).astype(F32).astype(BF16)
    rank = jnp.dot(chosen.astype(F32).astype(BF16), tri, preferred_element_type=F32)
    rank = jnp.where(chosen, rank - 1.0, -1.0)

    rank_out[...] = rank[half_n:groups]

    def pick(ranks):
        n = ranks.shape[0]
        c_iota = lax.broadcasted_iota(jnp.int32, (n, pair_cap, tok), 1).astype(F32)
        mask = ranks.reshape(n, 1, tok) == c_iota
        return mask.astype(F32).reshape(n * pair_cap, tok)

    def pack(ranks, src, dst, lo):
        n_part = ranks.shape[0]
        mat = pick(ranks).astype(BF16)
        for n in range(0, d_model, COLS):
            part = jnp.dot(mat, src[:, n:n + COLS], preferred_element_type=F32).astype(BF16)
            dst[lo:lo + n_part, :, n:n + COLS] = part.reshape(n_part, pair_cap, COLS)

    pl.semaphore_wait(barrier, groups - 1)

    @pl.when(inner == 1)
    def _():
        relay_in(1, 0).start()
        relay_in(0, 0).start()

    pack(rank[0:half_n], x_ref, send, 0)
    for idx in near_z + near_y:
        row_copy(idx).start()

    gd_row = lax.broadcasted_iota(jnp.int32, (groups * 8, tok), 0)
    gd_id = jnp.where(gd_row % 8 < local_count, (gd_row // 8) * local_count + gd_row % 8, -1)
    dense = jnp.zeros((groups * 8, tok), F32)
    for j in range(top_k):
        dense = dense + jnp.where(gd_id == slot_ids[j:j + 1, :], gates_ref[j:j + 1, :], 0.0)
    lane_iota = lax.broadcasted_iota(jnp.int32, (128, tok), 0).astype(F32)
    for s in range(groups):
        mat = (rank[s:s + 1, :] == lane_iota).astype(F32)
        sgate[s] = lax.dot_general(dense[s * 8:(s + 1) * 8], mat, (((1,), (1,)), ((), ())),
                                   precision=lax.Precision.HIGHEST, preferred_element_type=F32)
    for idx in far + near_z + near_y:
        gate_copy(idx).start()
    rgate[mine] = sgate[mine]
    recv[mine] = send[mine]

    for s in range(0, groups, quart):
        pick_t[s // quart] = pick(rank[s:s + quart]).T.astype(BF16)

    def relay(which):
        relay_in(1, which).wait_recv()
        relay_in(0, which).wait_recv()
        buf, lo = ((rel_send, 0), (send, half_n))[which]
        pack(rel_rank[which], rel_x.at[which], buf, lo)
        for slot in near_z + near_y:
            relay_copy(which, slot).start()
        recv[relayed[which]] = buf[lo + mine]

    @pl.when(inner == 1)
    def _():
        relay_in(1, 0).wait_send()
        relay_in(0, 0).wait_send()
        pl.semaphore_signal(go_sem, inc=1, device_id=device(near_z[0]), device_id_type=MESH_ID)
        for idx in far:
            gate_copy(idx).wait_send()
        relay(0)

    @pl.when(inner == 0)
    def _():
        for idx in far:
            gate_copy(idx).wait_send()
        pl.semaphore_wait(go_sem, 1)
        relay_in(1, 1).start()
        relay_in(0, 1).start()

    def ffn_pass(phase):
        lo = base[phase]
        turn = phases.index(phase)
        for j in range(quart):
            gcol[j * pair_cap:(j + 1) * pair_cap, :] = rgate[lo + j].T[0:pair_cap, :]

        def step(i, carry):
            expert = i if turn % 2 == 0 else local_count - 1 - i
            nxt = expert + 2 if turn % 2 == 0 else expert - 2
            slot = lax.rem(expert, 2)

            def refill(which):
                @pl.when(i < local_count - 2)
                def _():
                    w_copy(which, nxt, slot).start()

            def arrive(which):
                if turn == 0:
                    w_copy(which, expert, slot).wait()
                else:
                    @pl.when(i >= 2)
                    def _():
                        w_copy(which, expert, slot).wait()

            arrive(0)
            arrive(1)
            lhs = recv[pl.ds(lo, quart)].reshape(m, d_model)
            for n in range(0, ffn, COLS):
                w = min(COLS, ffn - n)
                g = jnp.dot(lhs, wg_buf[slot, :, n:n + w], preferred_element_type=F32)
                u = jnp.dot(lhs, wu_buf[slot, :, n:n + w], preferred_element_type=F32)
                hid[:, n:n + w] = (jax.nn.silu(g) * u).astype(BF16)
            refill(0)
            refill(1)
            arrive(2)
            gc = gcol[...]
            g_col = jnp.sum(jnp.where(lax.broadcasted_iota(jnp.int32, gc.shape, 1) == expert, gc, 0.0), axis=1, keepdims=True)
            hv = hid[...]
            for n in range(0, d_model, COLS):
                y = jnp.dot(hv, wd_buf[slot, :, n:n + COLS], preferred_element_type=F32).astype(BF16).astype(F32)
                acc[:, n:n + COLS] = acc[:, n:n + COLS] + jnp.where(g_col > 0.0, g_col * y, 0.0)
            refill(2)
            return carry

        acc[...] = jnp.zeros((m, d_model), F32)
        lax.fori_loop(0, local_count, step, 0)
        sums[pl.ds(lo, quart)] = acc[...].astype(BF16).reshape(quart, pair_cap, d_model)

    for phase in phases:
        if phase == 'q':
            pl.when(inner == 1)(lambda: relay(1))
        for idx in members[phase]:
            gate_copy(idx, arrival=True).wait_recv()
            if phase in ('p', 'g') and idx is members[phase][0]:
                pl.when(inner == 0)(lambda idx=idx: row_copy(idx, arrival=True).wait_recv())
            else:
                row_copy(idx, arrival=True).wait_recv()
        ffn_pass(phase)
        for idx in members[phase]:
            sum_copy(idx).start()
    ret[mine] = sums[mine]

    order = ('z', 'y', 'g', 'f')
    for phase in order:
        for idx in members[phase]:
            sum_copy(idx, arrival=True).wait_recv()
        lo = base[phase]
        got = ret[pl.ds(lo, quart)].reshape(m, d_model)
        pt = pick_t[lo // quart]
        for n in range(0, d_model, COLS):
            part = jnp.dot(pt, got[:, n:n + COLS], preferred_element_type=F32)
            if phase == order[0]:
                total[:, n:n + COLS] = x_ref[:, n:n + COLS].astype(F32) + part
            elif phase != order[-1]:
                total[:, n:n + COLS] = total[:, n:n + COLS] + part
            else:
                out_ref[:, n:n + COLS] = (total[:, n:n + COLS] + part).astype(BF16)

    for idx in others:
        sum_copy(idx).wait_send()
    for idx in near_y + near_z:
        row_copy(idx).wait_send()
        gate_copy(idx).wait_send()

    @pl.when(inner == 0)
    def _():
        relay_in(1, 1).wait_send()
        relay_in(0, 1).wait_send()

    @pl.when(inner == 1)
    def _():
        for slot in near_z + near_y:
            relay_copy(0, slot).wait_send()
            relay_copy(1, slot).wait_send()


def solution(mesh):
    groups = mesh.shape['ep']
    row_spec = P(('dp', 'ep'))
    expert_spec = P('ep')

    def device_step(tokens, expert_ids, gate_vals, w_gate, w_up, w_down):
        tok, top_k = expert_ids.shape
        d_model = tokens.shape[1]
        ffn = w_gate.shape[2]
        pair_cap = tok * (top_k // 2) // groups
        quart = groups // 4
        m = quart * pair_cap
        scratch = [pltpu.VMEM((groups, pair_cap, d_model), BF16) for _ in range(4)] + [
            pltpu.VMEM((groups, 8, 128), F32),
            pltpu.VMEM((groups, 8, 128), F32),
            pltpu.VMEM((m, 8), F32),
            pltpu.VMEM((4, tok, m), BF16),
            pltpu.VMEM((2, d_model, ffn), BF16),
            pltpu.VMEM((2, d_model, ffn), BF16),
            pltpu.VMEM((2, ffn, d_model), BF16),
            pltpu.VMEM((m, ffn), BF16),
            pltpu.VMEM((m, d_model), F32),
            pltpu.VMEM((tok, d_model), F32),
            pltpu.VMEM((groups // 2, tok), F32),
            pltpu.VMEM((2, groups // 2, tok), F32),
            pltpu.VMEM((2, tok, d_model), BF16),
            pltpu.VMEM((groups // 2, pair_cap, d_model), BF16),
            pltpu.SemaphoreType.DMA((3, 2)),
        ] + [pltpu.SemaphoreType.DMA((groups,)) for _ in range(6)] + [
            pltpu.SemaphoreType.DMA((2, groups // 2)), pltpu.SemaphoreType.DMA((2,)), pltpu.SemaphoreType.DMA((2, 2)), pltpu.SemaphoreType.REGULAR]
        vmem = pl.BlockSpec(memory_space=pltpu.VMEM)
        hbm = pl.BlockSpec(memory_space=pl.ANY)
        return pl.pallas_call(
            functools.partial(moe_kernel, groups, pair_cap),
            out_shape=jax.ShapeDtypeStruct((tok, d_model), BF16),
            in_specs=[vmem, vmem, vmem, hbm, hbm, hbm],
            out_specs=vmem,
            scratch_shapes=scratch,
            compiler_params=pltpu.CompilerParams(collective_id=0, has_side_effects=True, vmem_limit_bytes=66_000_000),
            name='moe_exchange',
        )(tokens, expert_ids.T, gate_vals.T, w_gate, w_up, w_down)

    return jax.shard_map(device_step, mesh=mesh, in_specs=(row_spec, row_spec, row_spec, expert_spec, expert_spec, expert_spec), out_specs=row_spec, check_vma=False)
```
